32 devices in a mesh: gx: 2 (over core), gy: 4 (over y, x), gz: 4 (over z).
Axes of the slice: x: 2, y: 2, z: 4, core: 2. Of those that a mesh axis runs over, the one named last changes fastest.
Arguments:
- field: float32 [256, 1024, 512], P('gz', 'gx', 'gy'), may hold values from -48 to 48
- factor_a: float32 [1024, 1024], replicated, may hold values from -0.5 to 3.5
- factor_b: float32 [512, 512], replicated, may hold values from -0.5 to 3.5
- factor_c: float32 [256, 256], replicated, may hold values from -0.5 to 3.5
Outputs:
- propagated: float32 [256, 1024, 512], P('gz', 'gx', 'gy')
The draws below stay inside these ranges and needn't reach their ends.
All inputs are finite; a program needn't handle non-finite values.
Results may differ from the reference program's by a relative error of at most 0.00007.
Values sent between devices are 32-bit elements; how exact they have to be, the bound alone decides.
A program may use at most 192 MiB of HBM per device.

```python
import math
import jax
import jax.numpy as jnp
from jax import lax

N1 = 1024
N2 = 512
N3 = 256


def draw_field(key, part):
    keys = jax.random.split(jax.random.fold_in(key, 10), 4)
    spread = math.log(2.2)
    rising = 0.5 * math.log(3.0)
    scale_three = jnp.exp(jax.random.uniform(keys[0], (N3,), jnp.float32, 0.0, spread) + rising * jnp.arange(N3, dtype=jnp.float32) / N3)
    scale_one = jnp.exp(jax.random.uniform(keys[1], (N1,), jnp.float32, 0.0, spread) + rising * jnp.arange(N1, dtype=jnp.float32) / N1)
    scale_two = jnp.exp(jax.random.uniform(keys[2], (N2,), jnp.float32, 0.0, spread) + rising * jnp.arange(N2, dtype=jnp.float32) / N2)
    noise = jax.random.truncated_normal(keys[3], -6.0, 6.0, (N3, N1, N2), jnp.float32)
    values = 0.25 * noise * scale_three[:, None, None] * scale_one[None, :, None] * scale_two[None, None, :]
    return jnp.clip(values, -48.0, 48.0)


def make_factor(key, order):
    keys = jax.random.split(key, 2)
    diagonal = jnp.exp(jax.random.uniform(keys[0], (order,), jnp.float32, 0.0, math.log(3.0)))
    off_part = jax.random.truncated_normal(keys[1], -4.0, 4.0, (order, order), jnp.float32) * 0.6 * order ** (-0.5)
    return off_part + jnp.diag(diagonal)


def draw_factor_a(key, part):
    return make_factor(jax.random.fold_in(key, 11), N1)


def draw_factor_b(key, part):
    return make_factor(jax.random.fold_in(key, 12), N2)


def draw_factor_c(key, part):
    return make_factor(jax.random.fold_in(key, 13), N3)


def setup_inputs(seed: int = 0) -> dict:
    splits = jax.random.split(jax.random.key(seed), 5)
    field = draw_field(jax.random.fold_in(splits[4], 71), 0)
    factor_a = draw_factor_a(jax.random.fold_in(splits[4], 71), 0)
    factor_b = draw_factor_b(jax.random.fold_in(splits[4], 71), 0)
    factor_c = draw_factor_c(jax.random.fold_in(splits[4], 71), 0)
    return {"field": field, "factor_a": factor_a, "factor_b": factor_b, "factor_c": factor_c}


epsilon = 1e-06
target_ratio = 0.5

def apply_operator(tensor, factor_a, factor_b, factor_c):
    highest = lax.Precision.HIGHEST
    along_one = jnp.einsum('ip,kpj->kij', factor_a, tensor, precision=highest)
    along_two = jnp.einsum('kip,jp->kij', tensor, factor_b, precision=highest)
    along_three = jnp.einsum('kp,pij->kij', factor_c, tensor, precision=highest)
    return along_one + along_two + along_three

def reference(field, factor_a, factor_b, factor_c):
    first_term = apply_operator(field, factor_a, factor_b, factor_c)
    size_field = jnp.sum(field * field)
    size_first = jnp.sum(first_term * first_term)
    step = target_ratio * jnp.sqrt(size_field / (size_first + epsilon))
    second_term = apply_operator(first_term, factor_a, factor_b, factor_c)
    return field - step * first_term + step * step / 2.0 * second_term
```

```python
import jax
import jax.numpy as jnp
from jax import lax
from jax.sharding import PartitionSpec as P

epsilon = 1e-06
target_ratio = 0.5


def on_device(field, factor_a, factor_b, factor_c):
    high = lax.Precision.HIGH
    count_x = lax.axis_size("gx")
    count_y = lax.axis_size("gy")
    me_x = lax.axis_index("gx")
    me_y = lax.axis_index("gy")
    paired = count_y & (count_y - 1) == 0

    def target(i, s, n, xor):
        return i ^ s if xor else (i + s) % n

    def source(i, s, n, xor):
        return i ^ s if xor else (i + n - s) % n

    def send(piece, s):
        if s == 0:
            return piece
        pairs = [(i, target(i, s, count_y, paired)) for i in range(count_y)]
        return lax.ppermute(piece, "gy", pairs)

    depth_home, width_one, width_two = field.shape
    depth = depth_home // count_y

    rows_a = lax.dynamic_slice_in_dim(factor_a, me_x * width_one, width_one, 0)
    blocks_a = [
        lax.dynamic_slice_in_dim(rows_a, ((me_x + count_x - s) % count_x) * width_one, width_one, 1)
        for s in range(count_x)
    ]
    blocks_b = jnp.concatenate(
        [
            jnp.concatenate(
                [
                    lax.dynamic_slice(
                        factor_b,
                        (
                            target(me_y, t, count_y, paired) * width_two,
                            source(me_y, s, count_y, paired) * width_two,
                        ),
                        (width_two, width_two),
                    )
                    for s in range(count_y)
                ],
                axis=1,
            )
            for t in range(count_y)
        ],
        axis=0,
    )

    def along_one(tensor):
        total = None
        for s in range(count_x):
            if s == 0:
                block = tensor
            else:
                pairs = [(i, (i + s) % count_x) for i in range(count_x)]
                block = lax.ppermute(tensor, "gx", pairs)
            term = jnp.einsum("ip,kpj->kij", blocks_a[s], block, precision=high)
            total = term if total is None else total + term
        return total

    def along_two(tensor):
        arrived = [
            send(
                lax.dynamic_slice_in_dim(tensor, target(me_y, s, count_y, paired) * depth, depth, 0), s
            )
            for s in range(count_y)
        ]
        whole = jnp.concatenate(arrived, axis=2)
        product = jnp.einsum("kip,jp->kij", whole, blocks_b, precision=high)
        result = jnp.zeros_like(tensor)
        for s in range(count_y):
            back = send(product[:, :, s * width_two : (s + 1) * width_two], s)
            result = lax.dynamic_update_slice_in_dim(
                result, back, source(me_y, s, count_y, paired) * depth, 0
            )
        return result

    count_z = lax.axis_size("gz")
    width_piece = width_one // count_z

    def to_fibres(tensor):
        pieces = tensor.reshape(depth_home, count_z, width_piece, width_two)
        pieces = pieces.transpose(1, 0, 2, 3).reshape(count_z * depth_home, width_piece, width_two)
        return lax.all_to_all(pieces, "gz", split_axis=0, concat_axis=0, tiled=True)

    def to_home(fibres):
        pieces = lax.all_to_all(fibres, "gz", split_axis=0, concat_axis=0, tiled=True)
        pieces = pieces.reshape(count_z, depth_home, width_piece, width_two)
        return pieces.transpose(1, 0, 2, 3).reshape(depth_home, width_one, width_two)

    def fibre_product(fibres):
        flat = fibres.reshape(fibres.shape[0], -1)
        return jnp.dot(factor_c, flat, precision=high).reshape(fibres.shape)

    fibres_one = fibre_product(to_fibres(field))
    fibres_two = fibre_product(fibres_one)
    planes = along_two(field) + along_one(field)
    home_one = to_home(fibres_one)
    first_term = planes + home_one
    mixed = planes + 2.0 * home_one
    home_two = to_home(fibres_two)
    second_term = along_two(mixed) + along_one(mixed) + home_two
    size_field, size_first = lax.psum(
        (jnp.sum(field * field), jnp.sum(first_term * first_term)), ("gx", "gy", "gz")
    )
    step = target_ratio * jnp.sqrt(size_field / (size_first + epsilon))
    return field - step * first_term + step * step / 2.0 * second_term


def solution(mesh):
    return jax.shard_map(
        on_device,
        mesh=mesh,
        in_specs=(P("gz", "gx", "gy"), P(), P(), P()),
        out_specs=P("gz", "gx", "gy"),
        check_vma=False,
    )
```
